32 devices in a mesh: grp: 2 (over x), mem: 16 (over z, y, core).
Axes of the slice: x: 2, y: 2, z: 4, core: 2. Of those that a mesh axis runs over, the one named last changes fastest.
Arguments:
- phi_owned: float32 [8, 8, 8, 4096], P(None, None, None, ('grp', 'mem')), may hold values from -6 to 6
- band_counts: int32 [2, 16], P('grp'), may hold values from 1 to 128, 512 in all within a row
- neighbours: int32 [2, 6, 512], P('grp'), may hold values from -1 to 1023, as said below
Outputs:
- phi_new: float32 [8, 8, 8, 4096], P(None, None, None, ('grp', 'mem'))
The draws below stay inside these ranges and needn't reach their ends.
Inputs may be any that keep to these rules, and one draw needn't show every extreme that they name: `band_counts`: in every group the counts sum to 512, each is at least 1, and the largest is exactly 128. `neighbours`: tile k of a group lies at column k mod 16 and row k // 16 of the group's tile sheet. An entry is -1 (no neighbour) or the id of the tile across that face: tile k - 1, k + 1, k - 16, k + 16 of the same group for faces 0 to 3 (never across an edge of the sheet), tile k of group g - 1 or g + 1 for faces 4 and 5. Links are mutual.
All inputs are finite; a program needn't handle non-finite values.
Results may differ from the reference program's by a relative error of at most 0.0003.
Values sent between devices are 32-bit elements; how exact they have to be, the bound alone decides.
A program may use at most 64 MiB of HBM per device.

```python
import math
import jax
import jax.numpy as jnp
import numpy as np
from jax import lax

TILE = 8
STEPS = 4
HOLD_DEV = 32
OWN_DEV = 128
COLUMNS = 16
GROUPS = 2
GROUP_TILES = 512
SLOTS = 4096


def draw_neighbours(key, part):
    tile_count = GROUP_TILES
    tile_ids = jnp.arange(tile_count, dtype=jnp.int32)
    column = tile_ids % COLUMNS
    sheet_row = tile_ids // COLUMNS
    group_index = jnp.arange(GROUPS, dtype=jnp.int32)[:, None]
    subkeys = jax.random.split(jax.random.fold_in(key, 7), 3)
    link_x = jax.random.randint(subkeys[0], (GROUPS, tile_count), 0, 4) < 3
    link_y = jax.random.randint(subkeys[1], (GROUPS, tile_count), 0, 4) < 3
    link_z = jax.random.randint(subkeys[2], (GROUPS, tile_count), 0, 4) < 3
    group_base = group_index * tile_count
    present = [(column > 0) & jnp.roll(link_x, 1, axis=1), (column < COLUMNS - 1) & link_x, (sheet_row > 0) & jnp.roll(link_y, COLUMNS, axis=1), (sheet_row < HOLD_DEV - 1) & link_y, (group_index > 0) & jnp.roll(link_z, 1, axis=0), (group_index < GROUPS - 1) & link_z]
    targets = [group_base + tile_ids - 1, group_base + tile_ids + 1, group_base + tile_ids - COLUMNS, group_base + tile_ids + COLUMNS, group_base - tile_count + tile_ids, group_base + tile_count + tile_ids]
    stacked = [jnp.where(linked, target, -1) for linked, target in zip(present, targets)]
    return jnp.stack(stacked, axis=1).astype(jnp.int32)


def block_scale(key, dims, cuts, smallest, high):
    level = 1.0
    for position, shards_of in cuts:
        heights = jax.random.uniform(jax.random.fold_in(jax.random.fold_in(key, 6), position), (shards_of,), jnp.float32, smallest / len(cuts), high / len(cuts))
        level = level * jnp.repeat(jnp.exp(heights), dims[position] // shards_of).reshape((-1,) + (1,) * (len(dims) - 1 - position))
    return level


def length_profile(amount, total, limit, lean):
    weights = [(1 << 20) // math.isqrt(grade ** lean) + 1 for grade in range(2, amount + 1)]
    spare, holding = total - limit - (amount - 1), [1] * (amount - 1)
    while spare > 0:
        movable = [i for i in range(amount - 1) if holding[i] < limit]
        mass, budget = sum([weights[i] for i in movable]), spare
        for i in movable:
            addition = min(limit - holding[i], max(1, budget * weights[i] // mass), spare)
            holding[i] = holding[i] + addition
            spare = spare - addition
    return np.array([limit] + holding)


def ragged_sizes(key, amount, total, bound, slope):
    if amount == 2:
        one = jax.random.randint(key, (), max(1, total - bound), min(bound, total - 1) + 1)
        return jnp.stack([one, total - one])
    sizes = jnp.asarray(length_profile(amount, total, bound, slope), jnp.int32)
    pairs = (amount - 1) // 2
    giver, sink = sizes[1:1 + 2 * pairs:2], sizes[2:2 + 2 * pairs:2]
    slack = jnp.minimum(giver - 1, bound - sink)
    passed = jax.random.randint(jax.random.fold_in(key, 1), (pairs,), 0, 1 << 20) % (slack + 1)
    sizes = sizes.at[1:1 + 2 * pairs:2].set(giver - passed).at[2:2 + 2 * pairs:2].set(sink + passed)
    return sizes[jax.random.permutation(jax.random.fold_in(key, 2), amount)]


def gaussian(rng, dims, spread, limit, shards=(), kind=jnp.bfloat16):
    values = jax.random.normal(rng, dims, jnp.float32) * spread
    if len(shards) > 0:
        values = block_scale(rng, dims, shards, -0.22, 0.18) * values
    return jnp.clip(values, min=-limit, max=limit).astype(kind)


def setup_inputs(seed: int = 0) -> dict:
    arg_keys = jax.random.split(jax.random.key(seed), 4)
    phi_owned = gaussian(arg_keys[0], (TILE, TILE, TILE, SLOTS), 1.0, 6.0, ((3, 32),), jnp.float32)
    band_counts = jax.vmap(lambda own: ragged_sizes(own, COLUMNS, GROUP_TILES, OWN_DEV, 2))(jax.random.split(arg_keys[1], GROUPS)).reshape((GROUPS, COLUMNS)).astype(jnp.int32)
    neighbours = draw_neighbours(jax.random.fold_in(arg_keys[3], 71), 0)
    return {"phi_owned": phi_owned, "band_counts": band_counts, "neighbours": neighbours}


TIME_STEP = 0.5
EPSILON = 1e-06

def upwind(backward, forward, positive):
    rising = jnp.maximum(jnp.square(jnp.maximum(backward, 0.0)), jnp.square(jnp.minimum(forward, 0.0)))
    falling = jnp.maximum(jnp.square(jnp.minimum(backward, 0.0)), jnp.square(jnp.maximum(forward, 0.0)))
    return jnp.where(positive, rising, falling)

def reference(phi_owned, band_counts, neighbours):
    tile_edge = phi_owned.shape[0]
    groups, columns = band_counts.shape
    tile_total = neighbours.shape[2]
    own_slots = phi_owned.shape[3] // (groups * columns)
    counts = band_counts.astype(jnp.int32)
    starts = (jnp.cumsum(counts, axis=1) - counts).astype(jnp.int32)
    tile_ids = jnp.arange(tile_total, dtype=jnp.int32)
    owner_mask = (starts[:, None, :] <= tile_ids[None, :, None]).astype(jnp.int32)
    owner_of = (lax.optimization_barrier(jnp.sum(owner_mask, axis=2)) - 1).astype(jnp.int32)
    first_tile = jnp.take_along_axis(starts, owner_of, axis=1).astype(jnp.int32)
    group_ids = jnp.arange(groups, dtype=jnp.int32)[:, None]
    slot_index = ((group_ids * columns + owner_of) * own_slots + tile_ids[None, :] - first_tile).reshape(-1).astype(jnp.int32)
    level_set = jnp.take(phi_owned, slot_index, axis=3)
    sign_field = level_set / jnp.sqrt(level_set * level_set + 1.0)
    positive = sign_field > 0
    link_table = jnp.transpose(neighbours, (1, 0, 2)).reshape(6, groups * tile_total)
    present = link_table >= 0
    safe_ids = jnp.maximum(link_table, 0).astype(jnp.int32)
    for sweep in range(STEPS):
        squares = jnp.zeros_like(level_set)
        for direction in range(3):
            low_layer = lax.index_in_dim(level_set, 0, direction, keepdims=True)
            high_layer = lax.index_in_dim(level_set, tile_edge - 1, direction, keepdims=True)
            below = jnp.where(present[2 * direction], jnp.take(high_layer, safe_ids[2 * direction], axis=3), low_layer)
            above = jnp.where(present[2 * direction + 1], jnp.take(low_layer, safe_ids[2 * direction + 1], axis=3), high_layer)
            extended = jnp.concatenate([below, level_set, above], axis=direction)
            backward = level_set - lax.slice_in_dim(extended, 0, tile_edge, axis=direction)
            forward = lax.slice_in_dim(extended, 2, tile_edge + 2, axis=direction) - level_set
            squares = squares + upwind(backward, forward, positive)
        level_set = level_set - TIME_STEP * sign_field * (jnp.sqrt(squares + EPSILON) - 1.0)
    return jnp.zeros_like(phi_owned).at[:, :, :, slot_index].set(level_set)
```

```python
import functools

import jax
import jax.numpy as jnp
from jax import lax
from jax.experimental import pallas as pl
from jax.experimental.pallas import tpu as pltpu
from jax.sharding import PartitionSpec as P

STEPS = 4
TIME_STEP = 0.5
EPSILON = 1e-06
LANES = 128
F32 = jnp.float32
BF16 = jnp.bfloat16


def roll(x, shift, axis):
    shift = shift % x.shape[axis]
    return x if shift == 0 else pltpu.roll(x, shift, axis)


def pieces(x, axis):
    high = x.astype(BF16)
    rest = x - high.astype(F32)
    middle = rest.astype(BF16)
    low = (rest - middle.astype(F32)).astype(BF16)
    return jnp.concatenate([high, middle, low], axis=axis)


def dot(a, b, dims):
    return lax.dot_general(a, b, (dims, ((), ())), preferred_element_type=F32)


def kernel(
    columns, groups, phi_hbm, counts_hbm, links_hbm, out_ref,
    phi_ref, counts_ref, links_own, links_below, links_above,
    leave, land, back, home, pack, up, down, from_below, from_above, from_left, from_right,
    level, sign, in_sem, out_send, out_recv, back_send, back_recv, side_send, side_recv,
):
    edge = phi_ref.shape[0]
    own_slots = phi_ref.shape[3]
    padded, tiles = leave.shape[1], links_own.shape[2]
    rows = tiles // columns
    halo = STEPS
    wide = 2 * edge
    layers = edge + 2 * halo
    me, grp = lax.axis_index("mem"), lax.axis_index("grp")
    has_left, has_right = me > 0, me < columns - 1
    has_below, has_above = grp > 0, grp < groups - 1
    across_grp = [(-1, has_below), (1, has_above)]
    across_mem = [(-1, has_left), (1, has_right)]
    distances = sorted(range(1, columns), key=lambda d: -min(d, columns - d))

    fetch = [
        pltpu.make_async_copy(phi_hbm, phi_ref, in_sem.at[0]),
        pltpu.make_async_copy(counts_hbm, counts_ref, in_sem.at[1]),
        pltpu.make_async_copy(links_hbm, links_own, in_sem.at[2]),
    ]
    for copy in fetch:
        copy.start()
    for ref in (from_below, from_above, from_left, from_right):
        ref[...] = jnp.zeros_like(ref)
    for ref in (links_below, links_above):
        ref[...] = jnp.full_like(ref, -1)

    barrier = pltpu.get_barrier_semaphore()

    def greet(**peer):
        pl.semaphore_signal(barrier, inc=1, device_id=peer, device_id_type=pl.DeviceIdType.MESH)

    for d in distances:
        greet(mem=lax.rem(me + d, columns))
    greetings = jnp.int32(columns - 1)
    for dg, there in across_grp:
        for dm, beside in across_mem + [(0, True)]:
            both = jnp.logical_and(there, beside)
            greetings = greetings + both.astype(jnp.int32)

            @pl.when(both)
            def _():
                greet(grp=grp + dg, mem=me + dm)

    def remote(source, target, send, recv, **peer):
        return pltpu.make_async_remote_copy(
            src_ref=source, dst_ref=target, send_sem=send, recv_sem=recv,
            device_id=peer, device_id_type=pl.DeviceIdType.MESH)

    def begin_exchange(source, target, send, recv):
        started = []
        for d in distances:
            peer = lax.rem(me + d, columns)
            copy = remote(source.at[peer], target.at[me], send.at[d], recv.at[d], mem=peer)
            copy.start()
            started.append(copy)
        target[me] = source[me]
        return started

    def end_exchange(source, target, send, recv):
        for d in reversed(distances):
            origin = lax.rem(me + columns - d, columns)
            remote(source.at[origin], target.at[origin], send.at[d], recv.at[d],
                   mem=origin).wait_recv()

    late = []

    def shift(index, condition, sources, copy):
        pl.when(condition)(copy.start)
        late.append((condition, copy))
        return lambda: pl.when(sources)(copy.wait_recv)

    fetch[1].wait()
    count_of = [counts_ref[0, m] for m in range(columns)]
    first, count = jnp.int32(0), jnp.int32(0)
    for m in range(columns):
        first = first + jnp.where(m < me, count_of[m], 0)
        count = count + jnp.where(m == me, count_of[m], 0)
    entries = columns * padded
    slot = lax.broadcasted_iota(jnp.int32, (1, own_slots), 1)
    key = (first + slot) % columns * padded + slot // columns
    chosen = lax.broadcasted_iota(jnp.int32, (entries, own_slots), 0) == key
    placing = jnp.where(chosen, 1.0, 0.0).astype(F32)

    fetch[0].wait()
    cells = jnp.concatenate(
        [phi_ref[2 * pair + k, y] for pair in range(edge // 2) for y in range(edge) for k in range(2)],
        axis=0)
    leave[...] = dot(jnp.concatenate([placing.astype(BF16)] * 3, axis=1), pieces(cells, 1),
                     ((1,), (1,))).reshape(leave.shape)
    fetch[2].wait()

    pl.semaphore_wait(barrier, greetings)
    sent = begin_exchange(leave, land, out_send, out_recv)
    tables = [
        shift(0, has_above, has_below, remote(
            links_own, links_below, side_send.at[0], side_recv.at[0], grp=grp + 1)),
        shift(1, has_below, has_above, remote(
            links_own, links_above, side_send.at[1], side_recv.at[1], grp=grp - 1)),
    ]

    def arrival(dims, axis):
        entry = lax.broadcasted_iota(jnp.int32, dims, axis)
        block, place = entry // padded, entry % padded
        start, length = jnp.zeros(dims, jnp.int32), jnp.zeros(dims, jnp.int32)
        for m in range(columns):
            start = start + jnp.where(block > m, count_of[m], 0)
            length = length + jnp.where(block == m, count_of[m], 0)
        shape = (rows, entries) if axis == 1 else (entries, rows)
        offset = lax.broadcasted_iota(jnp.int32, shape, 1 - axis) * columns + me - start
        begin = place * columns
        return jnp.where((offset >= begin) & (offset < begin + columns) & (offset < length),
                         1.0, 0.0).astype(F32).astype(BF16)

    arrive = jnp.concatenate([arrival((1, entries), 1)] * 3, axis=1)
    depart = jnp.concatenate([arrival((entries, 1), 0)] * 3, axis=1)
    living = jnp.concatenate([jnp.where(slot < count, placing, 0.0).astype(BF16)] * 3, axis=0)

    lane = lax.broadcasted_iota(jnp.int32, (rows, LANES), 1)
    z = lane % wide
    tile_of = (lax.broadcasted_iota(jnp.int32, (rows, tiles), 1)
               - lax.broadcasted_iota(jnp.int32, (rows, tiles), 0) * columns - me)
    held = {dm: tile_of == dm for dm in (-1, 0, 1)}

    for arrived in tables:
        arrived()

    def link(table, face, dm):
        there = jnp.where(table[face] >= 0, 1.0, 0.0).astype(F32)
        value = jnp.sum(jnp.where(held[dm], there, 0.0), axis=1, keepdims=True)
        return jnp.broadcast_to(value, (rows, LANES))

    def layered(face, dm):
        return jnp.where(z < halo, link(links_below, face, dm),
                         jnp.where(z >= halo + edge, link(links_above, face, dm),
                                   link(links_own, face, dm)))

    link_x = [layered(0, 0), layered(1, 0)]
    masks_y = [jnp.where(lane < wide, layered(2, dm), 1.0) for dm in (-1, 0, 1)]
    masks_z = [jnp.where(z == halo, link(links_own, 4, dm),
                         jnp.where(z == halo + edge, link(links_own, 5, dm),
                                   jnp.where(z == 0, 0.0, 1.0))) for dm in (-1, 0, 1)]

    end_exchange(leave, land, out_send, out_recv)
    packed = dot(arrive, pieces(land[...].reshape(-1, land.shape[2]), 0), ((1,), (0,)))
    pairs = [packed[:, p * LANES:(p + 1) * LANES] for p in range(edge // 2)]
    for p, both in enumerate(pairs):
        pack[p] = both
    low = lane % edge < halo
    slots = up.shape[0]
    for q in range(slots):
        here, after = pairs[2 * q], pairs[2 * q + 1]
        up[q] = jnp.where(low, roll(after, -halo, 1), here)
        down[q] = jnp.where(low, here, roll(after, halo, 1))

    half = edge // 4
    messages = []
    for dg, there, back_there, source, target, base in (
        (1, has_above, has_below, up, from_below, 2), (-1, has_below, has_above, down, from_above, 5),
    ):
        for k, (dm, beside, back_beside, part) in enumerate((
            (1, has_right, has_left, slots - 1), (-1, has_left, has_right, 0),
        )):
            messages.append(shift(
                base + k, jnp.logical_and(there, beside), jnp.logical_and(back_there, back_beside),
                remote(source.at[part], target.at[1 - dm, part], side_send.at[base + k],
                       side_recv.at[base + k], grp=grp + dg, mem=me + dm)))
        messages.append(shift(
            base + 2, there, back_there,
            remote(source, target.at[1], side_send.at[base + 2], side_recv.at[base + 2], grp=grp + dg)))
    messages.append(shift(8, has_right, has_left, remote(
        pack.at[pl.ds(half, half)], from_left, side_send.at[8], side_recv.at[8], mem=me + 1)))
    messages.append(shift(9, has_left, has_right, remote(
        pack.at[pl.ds(0, half)], from_right, side_send.at[9], side_recv.at[9], mem=me - 1)))

    for arrived in messages:
        arrived()

    for i in range(layers):
        x = i - halo
        region = 0 if x < 0 else (1 if x < edge else 2)
        x = x % edge
        p, k = divmod(x, 2)
        q, t = divmod(p, 2)
        own = pairs[p] if region == 1 else (from_left[p - half] if region == 0 else from_right[p])
        below = roll(from_below[region, q], -halo * (1 - t) - edge * k, 1)
        above = roll(from_above[region, q], edge + halo - edge * k - halo * t, 1)
        value = jnp.where(z < halo, below,
                          jnp.where(z >= halo + edge, above, roll(own, halo - edge * k, 1)))
        level[0, i] = value
        sign[i] = value / jnp.sqrt(value * value + 1.0)

    def sweep(step, low, high):
        now, later = step % 2, (step + 1) % 2
        gap = None
        for i in range(low, high):
            region = 0 if i < halo else (1 if i < halo + edge else 2)
            mask_y, mask_z = masks_y[region], masks_z[region]
            value, field = level[now, i], sign[i]
            side = jnp.where(field > 0, 1.0, -1.0)

            def across(j):
                change = level[now, j] - level[now, j - 1]
                if j == halo:
                    change = change * link_x[0]
                elif j == halo + edge:
                    change = change * link_x[1]
                return change

            gap = across(i) if gap is None else gap
            ahead = across(i + 1)
            most = jnp.maximum(jnp.maximum(side * gap, -(side * ahead)), 0.0)
            squares = most * most
            gap = ahead

            turned = roll(value, wide, 1)
            before = jnp.where(lane < wide, roll(turned, 1, 0), turned)
            behind = (value - before) * mask_y
            turned = roll(behind, -wide, 1)
            ahead = jnp.where(lane >= LANES - wide, roll(turned, -1, 0), turned)
            most = jnp.maximum(jnp.maximum(side * behind, -(side * ahead)), 0.0)
            squares = squares + most * most

            behind = (value - roll(value, 1, 1)) * mask_z
            ahead = roll(behind, -1, 1)
            most = jnp.maximum(jnp.maximum(side * behind, -(side * ahead)), 0.0)
            squares = squares + most * most
            level[later, i] = value - TIME_STEP * field * (jnp.sqrt(squares + EPSILON) - 1.0)

    for step in range(STEPS):
        sweep(step, step + 1, layers - 1 - step)

    last = STEPS % 2
    final = []
    for pair in range(edge // 2):
        one, two = level[last, halo + 2 * pair], level[last, halo + 2 * pair + 1]
        final.append(jnp.where(z < edge, roll(one, -halo, 1), roll(two, edge - halo, 1)))
    back[...] = dot(depart, pieces(jnp.concatenate(final, axis=1), 0),
                    ((1,), (0,))).reshape(back.shape)
    sent += begin_exchange(back, home, back_send, back_recv)
    end_exchange(back, home, back_send, back_recv)

    owned = dot(living, pieces(home[...].reshape(-1, home.shape[2]), 0), ((0,), (0,))).T
    for pair in range(edge // 2):
        for y in range(edge):
            for k in range(2):
                at = ((pair * edge + y) * 2 + k) * edge
                out_ref[2 * pair + k, y] = owned[at:at + edge]
    for copy in sent:
        copy.wait_send()
    for there, copy in late:
        pl.when(there)(copy.wait_send)


def on_device(phi_owned, band_counts, neighbours):
    edge, own_slots = phi_owned.shape[0], phi_owned.shape[3]
    columns, groups = lax.axis_size("mem"), lax.axis_size("grp")
    tiles = neighbours.shape[2]
    rows = tiles // columns
    padded = -(-own_slots // (8 * columns)) * 8
    halo, cells = STEPS, edge * edge * edge
    anywhere = pl.BlockSpec(memory_space=pl.ANY)
    buffer = pltpu.VMEM((columns, padded, cells), F32)
    table = pltpu.VMEM((6, 1, tiles), jnp.int32)
    pair = lambda *lead: pltpu.VMEM((*lead, rows, LANES), F32)
    slots, layers = edge // 4, edge + 2 * halo
    return pl.pallas_call(
        functools.partial(kernel, columns, groups),
        out_shape=jax.ShapeDtypeStruct(phi_owned.shape, F32),
        in_specs=[anywhere] * 3,
        out_specs=pl.BlockSpec(memory_space=pltpu.VMEM),
        scratch_shapes=[
            pltpu.VMEM(phi_owned.shape, F32), pltpu.SMEM(band_counts.shape, jnp.int32),
            table, table, table,
        ] + [buffer] * 4 + [
            pair(edge // 2), pair(slots), pair(slots), pair(3, slots), pair(3, slots),
            pair(edge // 4), pair(edge // 4), pair(2, layers), pair(layers),
            pltpu.SemaphoreType.DMA((3,)),
        ] + [pltpu.SemaphoreType.DMA((columns,))] * 4 + [pltpu.SemaphoreType.DMA((10,))] * 2,
        compiler_params=pltpu.CompilerParams(collective_id=0, has_side_effects=True),
    )(phi_owned, band_counts, jnp.transpose(neighbours, (1, 0, 2)))


def solution(mesh):
    return jax.shard_map(
        on_device,
        mesh=mesh,
        in_specs=(P(None, None, None, ("grp", "mem")), P("grp", None), P("grp", None, None)),
        out_specs=P(None, None, None, ("grp", "mem")),
        check_vma=False,
    )
```

```python
import functools

import jax
import jax.numpy as jnp
from jax import lax
from jax.experimental import pallas as pl
from jax.experimental.pallas import tpu as pltpu
from jax.sharding import PartitionSpec as P

STEPS = 4
TIME_STEP = 0.5
EPSILON = 1e-06
LANES = 128
F32 = jnp.float32
BF16 = jnp.bfloat16


def roll(x, shift, axis):
    shift = shift % x.shape[axis]
    return x if shift == 0 else pltpu.roll(x, shift, axis)


def pieces(x, axis):
    high = x.astype(BF16)
    rest = x - high.astype(F32)
    middle = rest.astype(BF16)
    low = (rest - middle.astype(F32)).astype(BF16)
    return jnp.concatenate([high, middle, low], axis=axis)


def dot(a, b, dims):
    return lax.dot_general(a, b, (dims, ((), ())), preferred_element_type=F32)


def kernel(
    columns, groups, phi_hbm, counts_hbm, links_hbm, out_ref,
    phi_ref, counts_ref, links_own, links_below, links_above,
    leave, land, back, home, pack, up, down, from_below, from_above, from_left, from_right,
    level, sign, in_sem, out_send, out_recv, back_send, back_recv, side_send, side_recv,
):
    edge = phi_ref.shape[0]
    own_slots = phi_ref.shape[3]
    padded, tiles = leave.shape[1], links_own.shape[2]
    rows = tiles // columns
    halo = STEPS
    wide = 2 * edge
    layers = edge + 2 * halo
    me, grp = lax.axis_index("mem"), lax.axis_index("grp")
    has_left, has_right = me > 0, me < columns - 1
    has_below, has_above = grp > 0, grp < groups - 1
    across_grp = [(-1, has_below), (1, has_above)]
    across_mem = [(-1, has_left), (1, has_right)]
    distances = range(1, columns)

    fetch = [
        pltpu.make_async_copy(phi_hbm, phi_ref, in_sem.at[0]),
        pltpu.make_async_copy(counts_hbm, counts_ref, in_sem.at[1]),
        pltpu.make_async_copy(links_hbm, links_own, in_sem.at[2]),
    ]
    for copy in fetch:
        copy.start()
    for ref in (from_below, from_above, from_left, from_right):
        ref[...] = jnp.zeros_like(ref)
    for ref in (links_below, links_above):
        ref[...] = jnp.full_like(ref, -1)

    barrier = pltpu.get_barrier_semaphore()

    def greet(**peer):
        pl.semaphore_signal(barrier, inc=1, device_id=peer, device_id_type=pl.DeviceIdType.MESH)

    for d in distances:
        greet(mem=lax.rem(me + d, columns))
    greetings = jnp.int32(columns - 1)
    for dg, there in across_grp:
        for dm, beside in across_mem + [(0, True)]:
            both = jnp.logical_and(there, beside)
            greetings = greetings + both.astype(jnp.int32)

            @pl.when(both)
            def _():
                greet(grp=grp + dg, mem=me + dm)

    def remote(source, target, send, recv, **peer):
        return pltpu.make_async_remote_copy(
            src_ref=source, dst_ref=target, send_sem=send, recv_sem=recv,
            device_id=peer, device_id_type=pl.DeviceIdType.MESH)

    def begin_exchange(source, target, send, recv):
        started = []
        for d in distances:
            peer = lax.rem(me + d, columns)
            copy = remote(source.at[peer], target.at[me], send.at[d], recv.at[d], mem=peer)
            copy.start()
            started.append(copy)
        target[me] = source[me]
        return started

    def end_exchange(source, target, send, recv):
        for d in reversed(distances):
            origin = lax.rem(me + columns - d, columns)
            remote(source.at[origin], target.at[origin], send.at[d], recv.at[d],
                   mem=origin).wait_recv()

    late = []

    def shift(index, condition, sources, copy):
        pl.when(condition)(copy.start)
        late.append((condition, copy))
        return lambda: pl.when(sources)(copy.wait_recv)

    fetch[1].wait()
    count_of = [counts_ref[0, m] for m in range(columns)]
    first, count = jnp.int32(0), jnp.int32(0)
    for m in range(columns):
        first = first + jnp.where(m < me, count_of[m], 0)
        count = count + jnp.where(m == me, count_of[m], 0)
    entries = columns * padded
    slot = lax.broadcasted_iota(jnp.int32, (1, own_slots), 1)
    key = (first + slot) % columns * padded + slot // columns
    chosen = lax.broadcasted_iota(jnp.int32, (entries, own_slots), 0) == key
    placing = jnp.where(chosen, 1.0, 0.0).astype(F32)

    fetch[0].wait()
    cells = jnp.concatenate(
        [phi_ref[2 * pair + k, y] for pair in range(edge // 2) for y in range(edge) for k in range(2)],
        axis=0)
    leave[...] = dot(jnp.concatenate([placing.astype(BF16)] * 3, axis=1), pieces(cells, 1),
                     ((1,), (1,))).reshape(leave.shape)
    fetch[2].wait()

    pl.semaphore_wait(barrier, greetings)
    sent = begin_exchange(leave, land, out_send, out_recv)
    tables = [
        shift(0, has_above, has_below, remote(
            links_own, links_below, side_send.at[0], side_recv.at[0], grp=grp + 1)),
        shift(1, has_below, has_above, remote(
            links_own, links_above, side_send.at[1], side_recv.at[1], grp=grp - 1)),
    ]

    def arrival(dims, axis):
        entry = lax.broadcasted_iota(jnp.int32, dims, axis)
        block, place = entry // padded, entry % padded
        start, length = jnp.zeros(dims, jnp.int32), jnp.zeros(dims, jnp.int32)
        for m in range(columns):
            start = start + jnp.where(block > m, count_of[m], 0)
            length = length + jnp.where(block == m, count_of[m], 0)
        shape = (rows, entries) if axis == 1 else (entries, rows)
        offset = lax.broadcasted_iota(jnp.int32, shape, 1 - axis) * columns + me - start
        begin = place * columns
        return jnp.where((offset >= begin) & (offset < begin + columns) & (offset < length),
                         1.0, 0.0).astype(F32).astype(BF16)

    arrive = jnp.concatenate([arrival((1, entries), 1)] * 3, axis=1)
    depart = jnp.concatenate([arrival((entries, 1), 0)] * 3, axis=1)
    living = jnp.concatenate([jnp.where(slot < count, placing, 0.0).astype(BF16)] * 3, axis=0)

    lane = lax.broadcasted_iota(jnp.int32, (rows, LANES), 1)
    z = lane % wide
    tile_of = (lax.broadcasted_iota(jnp.int32, (rows, tiles), 1)
               - lax.broadcasted_iota(jnp.int32, (rows, tiles), 0) * columns - me)
    held = {dm: tile_of == dm for dm in (-1, 0, 1)}

    for arrived in tables:
        arrived()

    def link(table, face, dm):
        there = jnp.where(table[face] >= 0, 1.0, 0.0).astype(F32)
        value = jnp.sum(jnp.where(held[dm], there, 0.0), axis=1, keepdims=True)
        return jnp.broadcast_to(value, (rows, LANES))

    def layered(face, dm):
        return jnp.where(z < halo, link(links_below, face, dm),
                         jnp.where(z >= halo + edge, link(links_above, face, dm),
                                   link(links_own, face, dm)))

    link_x = [layered(0, 0), layered(1, 0)]
    masks_y = [jnp.where(lane < wide, layered(2, dm), 1.0) for dm in (-1, 0, 1)]
    masks_z = [jnp.where(z == halo, link(links_own, 4, dm),
                         jnp.where(z == halo + edge, link(links_own, 5, dm),
                                   jnp.where(z == 0, 0.0, 1.0))) for dm in (-1, 0, 1)]

    end_exchange(leave, land, out_send, out_recv)
    packed = dot(arrive, pieces(land[...].reshape(-1, land.shape[2]), 0), ((1,), (0,)))
    pairs = [packed[:, p * LANES:(p + 1) * LANES] for p in range(edge // 2)]
    for p, both in enumerate(pairs):
        pack[p] = both
    low = lane % edge < halo
    slots = up.shape[0]
    for q in range(slots):
        here, after = pairs[2 * q], pairs[2 * q + 1]
        up[q] = jnp.where(low, roll(after, -halo, 1), here)
        down[q] = jnp.where(low, here, roll(after, halo, 1))

    half = edge // 4
    messages = []
    for dg, there, back_there, source, target, base in (
        (1, has_above, has_below, up, from_below, 2), (-1, has_below, has_above, down, from_above, 5),
    ):
        for k, (dm, beside, back_beside, part) in enumerate((
            (1, has_right, has_left, slots - 1), (-1, has_left, has_right, 0),
        )):
            messages.append(shift(
                base + k, jnp.logical_and(there, beside), jnp.logical_and(back_there, back_beside),
                remote(source.at[part], target.at[1 - dm, part], side_send.at[base + k],
                       side_recv.at[base + k], grp=grp + dg, mem=me + dm)))
        messages.append(shift(
            base + 2, there, back_there,
            remote(source, target.at[1], side_send.at[base + 2], side_recv.at[base + 2], grp=grp + dg)))
    messages.append(shift(8, has_right, has_left, remote(
        pack.at[pl.ds(half, half)], from_left, side_send.at[8], side_recv.at[8], mem=me + 1)))
    messages.append(shift(9, has_left, has_right, remote(
        pack.at[pl.ds(0, half)], from_right, side_send.at[9], side_recv.at[9], mem=me - 1)))

    for arrived in messages:
        arrived()

    for i in range(layers):
        x = i - halo
        region = 0 if x < 0 else (1 if x < edge else 2)
        x = x % edge
        p, k = divmod(x, 2)
        q, t = divmod(p, 2)
        own = pairs[p] if region == 1 else (from_left[p - half] if region == 0 else from_right[p])
        below = roll(from_below[region, q], -halo * (1 - t) - edge * k, 1)
        above = roll(from_above[region, q], edge + halo - edge * k - halo * t, 1)
        value = jnp.where(z < halo, below,
                          jnp.where(z >= halo + edge, above, roll(own, halo - edge * k, 1)))
        level[0, i] = value
        sign[i] = value / jnp.sqrt(value * value + 1.0)

    def sweep(step, low, high):
        now, later = step % 2, (step + 1) % 2
        gap = None
        for i in range(low, high):
            region = 0 if i < halo else (1 if i < halo + edge else 2)
            mask_y, mask_z = masks_y[region], masks_z[region]
            value, field = level[now, i], sign[i]
            side = jnp.where(field > 0, 1.0, -1.0)

            def across(j):
                change = level[now, j] - level[now, j - 1]
                if j == halo:
                    change = change * link_x[0]
                elif j == halo + edge:
                    change = change * link_x[1]
                return change

            gap = across(i) if gap is None else gap
            ahead = across(i + 1)
            most = jnp.maximum(jnp.maximum(side * gap, -(side * ahead)), 0.0)
            squares = most * most
            gap = ahead

            turned = roll(value, wide, 1)
            before = jnp.where(lane < wide, roll(turned, 1, 0), turned)
            behind = (value - before) * mask_y
            turned = roll(behind, -wide, 1)
            ahead = jnp.where(lane >= LANES - wide, roll(turned, -1, 0), turned)
            most = jnp.maximum(jnp.maximum(side * behind, -(side * ahead)), 0.0)
            squares = squares + most * most

            behind = (value - roll(value, 1, 1)) * mask_z
            ahead = roll(behind, -1, 1)
            most = jnp.maximum(jnp.maximum(side * behind, -(side * ahead)), 0.0)
            squares = squares + most * most
            level[later, i] = value - TIME_STEP * field * (jnp.sqrt(squares + EPSILON) - 1.0)

    for step in range(STEPS):
        sweep(step, step + 1, layers - 1 - step)

    last = STEPS % 2
    final = []
    for pair in range(edge // 2):
        one, two = level[last, halo + 2 * pair], level[last, halo + 2 * pair + 1]
        final.append(jnp.where(z < edge, roll(one, -halo, 1), roll(two, edge - halo, 1)))
    back[...] = dot(depart, pieces(jnp.concatenate(final, axis=1), 0),
                    ((1,), (0,))).reshape(back.shape)
    sent += begin_exchange(back, home, back_send, back_recv)
    end_exchange(back, home, back_send, back_recv)

    owned = dot(living, pieces(home[...].reshape(-1, home.shape[2]), 0), ((0,), (0,))).T
    for pair in range(edge // 2):
        for y in range(edge):
            for k in range(2):
                at = ((pair * edge + y) * 2 + k) * edge
                out_ref[2 * pair + k, y] = owned[at:at + edge]
    for copy in sent:
        copy.wait_send()
    for there, copy in late:
        pl.when(there)(copy.wait_send)


def on_device(phi_owned, band_counts, neighbours):
    edge, own_slots = phi_owned.shape[0], phi_owned.shape[3]
    columns, groups = lax.axis_size("mem"), lax.axis_size("grp")
    tiles = neighbours.shape[2]
    rows = tiles // columns
    padded = -(-own_slots // (8 * columns)) * 8
    halo, cells = STEPS, edge * edge * edge
    anywhere = pl.BlockSpec(memory_space=pltpu.HBM)
    buffer = pltpu.VMEM((columns, padded, cells), F32)
    table = pltpu.VMEM((6, 1, tiles), jnp.int32)
    pair = lambda *lead: pltpu.VMEM((*lead, rows, LANES), F32)
    slots, layers = edge // 4, edge + 2 * halo
    return pl.pallas_call(
        functools.partial(kernel, columns, groups),
        out_shape=jax.ShapeDtypeStruct(phi_owned.shape, F32),
        in_specs=[anywhere] * 3,
        out_specs=pl.BlockSpec(memory_space=pltpu.VMEM),
        scratch_shapes=[
            pltpu.VMEM(phi_owned.shape, F32), pltpu.SMEM(band_counts.shape, jnp.int32),
            table, table, table,
        ] + [buffer] * 4 + [
            pair(edge // 2), pair(slots), pair(slots), pair(3, slots), pair(3, slots),
            pair(edge // 4), pair(edge // 4), pair(2, layers), pair(layers),
            pltpu.SemaphoreType.DMA((3,)),
        ] + [pltpu.SemaphoreType.DMA((columns,))] * 4 + [pltpu.SemaphoreType.DMA((10,))] * 2,
        compiler_params=pltpu.CompilerParams(
            collective_id=0, has_side_effects=True, vmem_limit_bytes=16 * 1024 * 1024),
    )(*[pltpu.with_memory_space_constraint(x, pltpu.HBM)
        for x in (phi_owned, band_counts, jnp.transpose(neighbours, (1, 0, 2)))])


def solution(mesh):
    return jax.shard_map(
        on_device,
        mesh=mesh,
        in_specs=(P(None, None, None, ("grp", "mem")), P("grp", None), P("grp", None, None)),
        out_specs=P(None, None, None, ("grp", "mem")),
        check_vma=False,
    )
```

```python
import functools

import jax
import jax.numpy as jnp
from jax import lax
from jax.experimental import pallas as pl
from jax.experimental.pallas import tpu as pltpu
from jax.sharding import PartitionSpec as P

STEPS = 4
TIME_STEP = 0.5
EPSILON = 1e-06
LANES = 128
F32 = jnp.float32
BF16 = jnp.bfloat16


def roll(x, shift, axis):
    shift = shift % x.shape[axis]
    return x if shift == 0 else pltpu.roll(x, shift, axis)


def pieces(x, axis):
    high = x.astype(BF16)
    rest = x - high.astype(F32)
    middle = rest.astype(BF16)
    low = (rest - middle.astype(F32)).astype(BF16)
    return jnp.concatenate([high, middle, low], axis=axis)


def dot(a, b, dims):
    return lax.dot_general(a, b, (dims, ((), ())), preferred_element_type=F32)


def kernel(
    columns, groups, phi_hbm, counts_hbm, links_hbm, out_ref,
    phi_ref, counts_ref, links_own, links_below, links_above,
    leave, land, back, home, pack, up, down, from_below, from_above, from_left, from_right,
    level, sign, turned, in_sem, out_send, out_recv, back_send, back_recv, side_send, side_recv,
):
    edge = phi_ref.shape[0]
    own_slots = phi_ref.shape[3]
    padded, tiles = leave.shape[1], links_own.shape[2]
    rows = tiles // columns
    halo = STEPS
    wide = 2 * edge
    layers = edge + 2 * halo
    me, grp = lax.axis_index("mem"), lax.axis_index("grp")
    has_left, has_right = me > 0, me < columns - 1
    has_below, has_above = grp > 0, grp < groups - 1
    across_grp = [(-1, has_below), (1, has_above)]
    across_mem = [(-1, has_left), (1, has_right)]
    distances = range(1, columns)

    fetch = [
        pltpu.make_async_copy(phi_hbm, phi_ref, in_sem.at[0]),
        pltpu.make_async_copy(counts_hbm, counts_ref, in_sem.at[1]),
        pltpu.make_async_copy(links_hbm, links_own, in_sem.at[2]),
    ]
    for copy in fetch:
        copy.start()
    for ref in (from_below, from_above, from_left, from_right):
        ref[...] = jnp.zeros_like(ref)
    for ref in (links_below, links_above):
        ref[...] = jnp.full_like(ref, -1)

    barrier = pltpu.get_barrier_semaphore()

    def greet(**peer):
        pl.semaphore_signal(barrier, inc=1, device_id=peer, device_id_type=pl.DeviceIdType.MESH)

    for d in distances:
        greet(mem=lax.rem(me + d, columns))
    greetings = jnp.int32(columns - 1)
    for dg, there in across_grp:
        for dm, beside in across_mem + [(0, True)]:
            both = jnp.logical_and(there, beside)
            greetings = greetings + both.astype(jnp.int32)

            @pl.when(both)
            def _():
                greet(grp=grp + dg, mem=me + dm)

    def remote(source, target, send, recv, **peer):
        return pltpu.make_async_remote_copy(
            src_ref=source, dst_ref=target, send_sem=send, recv_sem=recv,
            device_id=peer, device_id_type=pl.DeviceIdType.MESH)

    def begin_exchange(source, target, send, recv):
        started = []
        for d in distances:
            peer = lax.rem(me + d, columns)
            copy = remote(source.at[peer], target.at[me], send.at[d], recv.at[d], mem=peer)
            copy.start()
            started.append(copy)
        target[me] = source[me]
        return started

    def end_exchange(source, target, send, recv):
        for d in reversed(distances):
            origin = lax.rem(me + columns - d, columns)
            remote(source.at[origin], target.at[origin], send.at[d], recv.at[d],
                   mem=origin).wait_recv()

    late = []

    def shift(index, condition, sources, copy):
        pl.when(condition)(copy.start)
        late.append((condition, copy))
        return lambda: pl.when(sources)(copy.wait_recv)

    fetch[1].wait()
    count_of = [counts_ref[0, m] for m in range(columns)]
    first, count = jnp.int32(0), jnp.int32(0)
    for m in range(columns):
        first = first + jnp.where(m < me, count_of[m], 0)
        count = count + jnp.where(m == me, count_of[m], 0)
    entries = columns * padded
    slot = lax.broadcasted_iota(jnp.int32, (1, own_slots), 1)
    key = (first + slot) % columns * padded + slot // columns
    chosen = lax.broadcasted_iota(jnp.int32, (entries, own_slots), 0) == key
    placing = jnp.where(chosen, 1.0, 0.0).astype(F32)

    fetch[0].wait()
    cells = jnp.concatenate(
        [phi_ref[2 * pair + k, y] for pair in range(edge // 2) for y in range(edge) for k in range(2)],
        axis=0)
    leave[...] = dot(jnp.concatenate([placing.astype(BF16)] * 3, axis=1), pieces(cells, 1),
                     ((1,), (1,))).reshape(leave.shape)
    fetch[2].wait()

    pl.semaphore_wait(barrier, greetings)
    sent = begin_exchange(leave, land, out_send, out_recv)
    tables = [
        shift(0, has_above, has_below, remote(
            links_own, links_below, side_send.at[0], side_recv.at[0], grp=grp + 1)),
        shift(1, has_below, has_above, remote(
            links_own, links_above, side_send.at[1], side_recv.at[1], grp=grp - 1)),
    ]

    def arrival(dims, axis):
        entry = lax.broadcasted_iota(jnp.int32, dims, axis)
        block, place = entry // padded, entry % padded
        start, length = jnp.zeros(dims, jnp.int32), jnp.zeros(dims, jnp.int32)
        for m in range(columns):
            start = start + jnp.where(block > m, count_of[m], 0)
            length = length + jnp.where(block == m, count_of[m], 0)
        shape = (rows, entries) if axis == 1 else (entries, rows)
        offset = lax.broadcasted_iota(jnp.int32, shape, 1 - axis) * columns + me - start
        begin = place * columns
        return jnp.where((offset >= begin) & (offset < begin + columns) & (offset < length),
                         1.0, 0.0).astype(F32).astype(BF16)

    arrive = jnp.concatenate([arrival((1, entries), 1)] * 3, axis=1)
    depart = jnp.concatenate([arrival((entries, 1), 0)] * 3, axis=1)
    living = jnp.concatenate([jnp.where(slot < count, placing, 0.0).astype(BF16)] * 3, axis=0)

    lane = lax.broadcasted_iota(jnp.int32, (rows, LANES), 1)
    z = lane % wide
    tile_of = (lax.broadcasted_iota(jnp.int32, (rows, tiles), 1)
               - lax.broadcasted_iota(jnp.int32, (rows, tiles), 0) * columns - me)
    held = {dm: tile_of == dm for dm in (-1, 0, 1)}

    for arrived in tables:
        arrived()

    def link(table, face, dm):
        there = jnp.where(table[face] >= 0, 1.0, 0.0).astype(F32)
        value = jnp.sum(jnp.where(held[dm], there, 0.0), axis=1, keepdims=True)
        return jnp.broadcast_to(value, (rows, LANES))

    def layered(face, dm):
        return jnp.where(z < halo, link(links_below, face, dm),
                         jnp.where(z >= halo + edge, link(links_above, face, dm),
                                   link(links_own, face, dm)))

    link_x = [layered(0, 0), layered(1, 0)]
    masks_y = [jnp.where(lane < wide, layered(2, dm), 1.0) for dm in (-1, 0, 1)]
    masks_z = [jnp.where(z == halo, link(links_own, 4, dm),
                         jnp.where(z == halo + edge, link(links_own, 5, dm),
                                   jnp.where(z == 0, 0.0, 1.0))) for dm in (-1, 0, 1)]

    end_exchange(leave, land, out_send, out_recv)
    packed = dot(arrive, pieces(land[...].reshape(-1, land.shape[2]), 0), ((1,), (0,)))
    pairs = [packed[:, p * LANES:(p + 1) * LANES] for p in range(edge // 2)]
    for p, both in enumerate(pairs):
        pack[p] = both
    low = lane % edge < halo
    slots = up.shape[0]
    for q in range(slots):
        here, after = pairs[2 * q], pairs[2 * q + 1]
        up[q] = jnp.where(low, roll(after, -halo, 1), here)
        down[q] = jnp.where(low, here, roll(after, halo, 1))

    half = edge // 4
    messages = []
    for dg, there, back_there, source, target, base in (
        (1, has_above, has_below, up, from_below, 2), (-1, has_below, has_above, down, from_above, 5),
    ):
        for k, (dm, beside, back_beside, part) in enumerate((
            (1, has_right, has_left, slots - 1), (-1, has_left, has_right, 0),
        )):
            messages.append(shift(
                base + k, jnp.logical_and(there, beside), jnp.logical_and(back_there, back_beside),
                remote(source.at[part], target.at[1 - dm, part], side_send.at[base + k],
                       side_recv.at[base + k], grp=grp + dg, mem=me + dm)))
        messages.append(shift(
            base + 2, there, back_there,
            remote(source, target.at[1], side_send.at[base + 2], side_recv.at[base + 2], grp=grp + dg)))
    messages.append(shift(8, has_right, has_left, remote(
        pack.at[pl.ds(half, half)], from_left, side_send.at[8], side_recv.at[8], mem=me + 1)))
    messages.append(shift(9, has_left, has_right, remote(
        pack.at[pl.ds(0, half)], from_right, side_send.at[9], side_recv.at[9], mem=me - 1)))

    for arrived in messages:
        arrived()

    for i in range(layers):
        x = i - halo
        region = 0 if x < 0 else (1 if x < edge else 2)
        x = x % edge
        p, k = divmod(x, 2)
        q, t = divmod(p, 2)
        own = pairs[p] if region == 1 else (from_left[p - half] if region == 0 else from_right[p])
        below = roll(from_below[region, q], -halo * (1 - t) - edge * k, 1)
        above = roll(from_above[region, q], edge + halo - edge * k - halo * t, 1)
        value = jnp.where(z < halo, below,
                          jnp.where(z >= halo + edge, above, roll(own, halo - edge * k, 1)))
        level[0, i] = value
        sign[i] = value * lax.rsqrt(value * value + 1.0)

    always = me < columns

    def row_ahead(x):
        return jnp.where(lane >= LANES - wide, roll(x, -1, 0), x)

    ahead_y = [row_ahead(roll(mask, -wide, 1)) for mask in masks_y]
    ahead_z = [roll(mask, -1, 1) for mask in masks_z]

    def steepest(side, behind, ahead):
        most = jnp.maximum(jnp.maximum(side * behind, -(side * ahead)), 0.0)
        return most * most

    def sweep(step, low, high):
        now, later = step % 2, (step + 1) % 2

        @pl.when(always)
        def _():
            for k, shift_by in enumerate((wide, -wide, 1, -1)):
                for i in range(low, high):
                    turned[k, i] = roll(level[now, i], shift_by, 1)

        @pl.when(always)
        def _():
            gap = None
            for i in range(low, high):
                region = 0 if i < halo else (1 if i < halo + edge else 2)
                value, field = level[now, i], sign[i]
                side = jnp.where(field > 0, 1.0, -1.0)

                def across(j):
                    change = level[now, j] - level[now, j - 1]
                    if j == halo:
                        change = change * link_x[0]
                    elif j == halo + edge:
                        change = change * link_x[1]
                    return change

                gap = across(i) if gap is None else gap
                ahead = across(i + 1)
                squares = steepest(side, gap, ahead)
                gap = ahead
                before = turned[0, i]
                before = jnp.where(lane < wide, roll(before, 1, 0), before)
                squares = squares + steepest(side, (value - before) * masks_y[region],
                                             (row_ahead(turned[1, i]) - value) * ahead_y[region])
                squares = squares + steepest(side, (value - turned[2, i]) * masks_z[region],
                                             (turned[3, i] - value) * ahead_z[region]) + EPSILON
                level[later, i] = value - TIME_STEP * field * (squares * lax.rsqrt(squares) - 1.0)

    for step in range(STEPS):
        sweep(step, step + 1, layers - 1 - step)

    last = STEPS % 2
    final = []
    for pair in range(edge // 2):
        one, two = level[last, halo + 2 * pair], level[last, halo + 2 * pair + 1]
        final.append(jnp.where(z < edge, roll(one, -halo, 1), roll(two, edge - halo, 1)))
    back[...] = dot(depart, pieces(jnp.concatenate(final, axis=1), 0),
                    ((1,), (0,))).reshape(back.shape)
    sent += begin_exchange(back, home, back_send, back_recv)
    end_exchange(back, home, back_send, back_recv)

    owned = dot(living, pieces(home[...].reshape(-1, home.shape[2]), 0), ((0,), (0,))).T
    for pair in range(edge // 2):
        for y in range(edge):
            for k in range(2):
                at = ((pair * edge + y) * 2 + k) * edge
                out_ref[2 * pair + k, y] = owned[at:at + edge]
    for copy in sent:
        copy.wait_send()
    for there, copy in late:
        pl.when(there)(copy.wait_send)


def on_device(phi_owned, band_counts, neighbours):
    edge, own_slots = phi_owned.shape[0], phi_owned.shape[3]
    columns, groups = lax.axis_size("mem"), lax.axis_size("grp")
    tiles = neighbours.shape[2]
    rows = tiles // columns
    padded = -(-own_slots // (8 * columns)) * 8
    halo, cells = STEPS, edge * edge * edge
    anywhere = pl.BlockSpec(memory_space=pltpu.HBM)
    buffer = pltpu.VMEM((columns, padded, cells), F32)
    table = pltpu.VMEM((6, 1, tiles), jnp.int32)
    pair = lambda *lead: pltpu.VMEM((*lead, rows, LANES), F32)
    slots, layers = edge // 4, edge + 2 * halo
    return pl.pallas_call(
        functools.partial(kernel, columns, groups),
        out_shape=jax.ShapeDtypeStruct(phi_owned.shape, F32),
        in_specs=[anywhere] * 3,
        out_specs=pl.BlockSpec(memory_space=pltpu.VMEM),
        scratch_shapes=[
            pltpu.VMEM(phi_owned.shape, F32), pltpu.SMEM(band_counts.shape, jnp.int32),
            table, table, table,
        ] + [buffer] * 4 + [
            pair(edge // 2), pair(slots), pair(slots), pair(3, slots), pair(3, slots),
            pair(edge // 4), pair(edge // 4), pair(2, layers), pair(layers), pair(4, layers),
            pltpu.SemaphoreType.DMA((3,)),
        ] + [pltpu.SemaphoreType.DMA((columns,))] * 4 + [pltpu.SemaphoreType.DMA((10,))] * 2,
        compiler_params=pltpu.CompilerParams(
            collective_id=0, has_side_effects=True, vmem_limit_bytes=16 * 1024 * 1024),
    )(*[pltpu.with_memory_space_constraint(x, pltpu.HBM)
        for x in (phi_owned, band_counts, jnp.transpose(neighbours, (1, 0, 2)))])


def solution(mesh):
    return jax.shard_map(
        on_device,
        mesh=mesh,
        in_specs=(P(None, None, None, ("grp", "mem")), P("grp", None), P("grp", None, None)),
        out_specs=P(None, None, None, ("grp", "mem")),
        check_vma=False,
    )
```

```python
import functools

import jax
import jax.numpy as jnp
from jax import lax
from jax.experimental import pallas as pl
from jax.experimental.pallas import tpu as pltpu
from jax.sharding import PartitionSpec as P

STEPS = 4
TIME_STEP = 0.5
EPSILON = 1e-06
LANES = 128
F32 = jnp.float32
BF16 = jnp.bfloat16


def roll(x, shift, axis):
    shift = shift % x.shape[axis]
    return x if shift == 0 else pltpu.roll(x, shift, axis)


def pieces(x, axis):
    high = x.astype(BF16)
    rest = x - high.astype(F32)
    middle = rest.astype(BF16)
    low = (rest - middle.astype(F32)).astype(BF16)
    return jnp.concatenate([high, middle, low], axis=axis)


def dot(a, b, dims):
    return lax.dot_general(a, b, (dims, ((), ())), preferred_element_type=F32)


def kernel(
    columns, groups, phi_hbm, counts_hbm, links_hbm, out_ref,
    phi_ref, counts_ref, links_own, links_below, links_above,
    leave, land, back, home, pack, up, down, from_below, from_above, from_left, from_right,
    level, sign, turned, in_sem, out_send, out_recv, back_send, back_recv, side_send, side_recv,
):
    edge = phi_ref.shape[0]
    own_slots = phi_ref.shape[3]
    padded, tiles = leave.shape[1], links_own.shape[2]
    rows = tiles // columns
    halo = STEPS
    wide = 2 * edge
    layers = edge + 2 * halo
    me, grp = lax.axis_index("mem"), lax.axis_index("grp")
    has_left, has_right = me > 0, me < columns - 1
    has_below, has_above = grp > 0, grp < groups - 1
    across_grp = [(-1, has_below), (1, has_above)]
    across_mem = [(-1, has_left), (1, has_right)]
    distances = range(1, columns)

    fetch = [
        pltpu.make_async_copy(phi_hbm, phi_ref, in_sem.at[0]),
        pltpu.make_async_copy(counts_hbm, counts_ref, in_sem.at[1]),
        pltpu.make_async_copy(links_hbm, links_own, in_sem.at[2]),
    ]
    for copy in fetch:
        copy.start()

    barrier = pltpu.get_barrier_semaphore()

    def greet(**peer):
        pl.semaphore_signal(barrier, inc=1, device_id=peer, device_id_type=pl.DeviceIdType.MESH)

    for d in sorted(distances, key=lambda d: -min(d, columns - d)):
        greet(mem=lax.rem(me + d, columns))
    greetings = jnp.int32(columns - 1)
    for dg, there in across_grp:
        for dm, beside in across_mem + [(0, True)]:
            both = jnp.logical_and(there, beside)
            greetings = greetings + both.astype(jnp.int32)

            @pl.when(both)
            def _():
                greet(grp=grp + dg, mem=me + dm)

    def remote(source, target, send, recv, **peer):
        return pltpu.make_async_remote_copy(
            src_ref=source, dst_ref=target, send_sem=send, recv_sem=recv,
            device_id=peer, device_id_type=pl.DeviceIdType.MESH)

    early = 2

    def turn(i, favour):
        if not favour:
            return lax.rem(me + 1 + i, columns)
        if i == 0:
            return jnp.where(me == 0, 1, 0)
        rest = early + lax.rem(me + columns - 3 * early + i + 1, columns - early)
        return jnp.where(me < early, i + 1, 1 if i == 1 else rest)

    def begin_exchange(source, target, send, recv, favour=False):
        started = []
        for i in range(columns - 1):
            peer = turn(i, favour)
            d = lax.rem(peer - me + columns, columns)
            copy = remote(source.at[peer], target.at[me], send.at[d], recv.at[d], mem=peer)
            copy.start()
            started.append(copy)
        target[me] = source[me]
        return started

    def end_exchange(source, target, send, recv):
        for d in reversed(distances):
            origin = lax.rem(me + columns - d, columns)
            remote(source.at[origin], target.at[origin], send.at[d], recv.at[d],
                   mem=origin).wait_recv()

    late = []

    def shift(index, condition, sources, copy):
        pl.when(condition)(copy.start)
        late.append((condition, copy))
        return lambda: pl.when(sources)(copy.wait_recv)

    fetch[1].wait()
    count_of = [counts_ref[0, m] for m in range(columns)]
    first, count = jnp.int32(0), jnp.int32(0)
    for m in range(columns):
        first = first + jnp.where(m < me, count_of[m], 0)
        count = count + jnp.where(m == me, count_of[m], 0)
    entries = columns * padded
    slot = lax.broadcasted_iota(jnp.int32, (1, own_slots), 1)
    key = (first + slot) % columns * padded + slot // columns
    chosen = lax.broadcasted_iota(jnp.int32, (entries, own_slots), 0) == key
    placing = jnp.where(chosen, 1.0, 0.0).astype(F32)

    fetch[0].wait()
    cells = jnp.concatenate(
        [phi_ref[2 * pair + k, y] for pair in range(edge // 2) for y in range(edge) for k in range(2)],
        axis=0)
    leave[...] = dot(jnp.concatenate([placing.astype(BF16)] * 3, axis=1), pieces(cells, 1),
                     ((1,), (1,))).reshape(leave.shape)
    fetch[2].wait()

    pl.semaphore_wait(barrier, greetings)
    sent = begin_exchange(leave, land, out_send, out_recv)
    tables = [
        shift(0, has_above, has_below, remote(
            links_own, links_below, side_send.at[0], side_recv.at[0], grp=grp + 1)),
        shift(1, has_below, has_above, remote(
            links_own, links_above, side_send.at[1], side_recv.at[1], grp=grp - 1)),
    ]

    def blank(absent, *views):
        @pl.when(jnp.logical_not(absent))
        def _():
            for ref, value in views:
                ref[...] = jnp.full_like(ref, value)

    blank(has_left, (from_left, 0.0))
    blank(has_right, (from_right, 0.0))
    for there, table, ref in ((has_below, links_below, from_below), (has_above, links_above, from_above)):
        blank(there, (table, -1), (ref.at[1], 0.0))
        blank(jnp.logical_and(there, has_left), (ref.at[0], 0.0))
        blank(jnp.logical_and(there, has_right), (ref.at[2], 0.0))

    def arrival(dims, axis):
        entry = lax.broadcasted_iota(jnp.int32, dims, axis)
        block, place = entry // padded, entry % padded
        start, length = jnp.zeros(dims, jnp.int32), jnp.zeros(dims, jnp.int32)
        for m in range(columns):
            start = start + jnp.where(block > m, count_of[m], 0)
            length = length + jnp.where(block == m, count_of[m], 0)
        shape = (rows, entries) if axis == 1 else (entries, rows)
        offset = lax.broadcasted_iota(jnp.int32, shape, 1 - axis) * columns + me - start
        begin = place * columns
        return jnp.where((offset >= begin) & (offset < begin + columns) & (offset < length),
                         1.0, 0.0).astype(F32).astype(BF16)

    arrive = jnp.concatenate([arrival((1, entries), 1)] * 3, axis=1)
    depart = jnp.concatenate([arrival((entries, 1), 0)] * 3, axis=1)
    living = jnp.concatenate([jnp.where(slot < count, placing, 0.0).astype(BF16)] * 3, axis=0)

    lane = lax.broadcasted_iota(jnp.int32, (rows, LANES), 1)
    z = lane % wide
    tile_of = (lax.broadcasted_iota(jnp.int32, (rows, tiles), 1)
               - lax.broadcasted_iota(jnp.int32, (rows, tiles), 0) * columns - me)
    held = {dm: tile_of == dm for dm in (-1, 0, 1)}

    for arrived in tables:
        arrived()

    def link(table, face, dm):
        there = jnp.where(table[face] >= 0, 1.0, 0.0).astype(F32)
        value = jnp.sum(jnp.where(held[dm], there, 0.0), axis=1, keepdims=True)
        return jnp.broadcast_to(value, (rows, LANES))

    def layered(face, dm):
        return jnp.where(z < halo, link(links_below, face, dm),
                         jnp.where(z >= halo + edge, link(links_above, face, dm),
                                   link(links_own, face, dm)))

    link_x = [layered(0, 0), layered(1, 0)]
    masks_y = [jnp.where(lane < wide, layered(2, dm), 1.0) for dm in (-1, 0, 1)]
    masks_z = [jnp.where(z == halo, link(links_own, 4, dm),
                         jnp.where(z == halo + edge, link(links_own, 5, dm),
                                   jnp.where(z == 0, 0.0, 1.0))) for dm in (-1, 0, 1)]

    end_exchange(leave, land, out_send, out_recv)
    packed = dot(arrive, pieces(land[...].reshape(-1, land.shape[2]), 0), ((1,), (0,)))
    pairs = [packed[:, p * LANES:(p + 1) * LANES] for p in range(edge // 2)]
    for p, both in enumerate(pairs):
        pack[p] = both
    low = lane % edge < halo
    slots = up.shape[0]
    for q in range(slots):
        here, after = pairs[2 * q], pairs[2 * q + 1]
        up[q] = jnp.where(low, roll(after, -halo, 1), here)
        down[q] = jnp.where(low, here, roll(after, halo, 1))

    half = edge // 4
    messages = []
    for dg, there, back_there, source, target, base in (
        (1, has_above, has_below, up, from_below, 2), (-1, has_below, has_above, down, from_above, 5),
    ):
        for k, (dm, beside, back_beside, part) in enumerate((
            (1, has_right, has_left, slots - 1), (-1, has_left, has_right, 0),
        )):
            messages.append(shift(
                base + k, jnp.logical_and(there, beside), jnp.logical_and(back_there, back_beside),
                remote(source.at[part], target.at[1 - dm, part], side_send.at[base + k],
                       side_recv.at[base + k], grp=grp + dg, mem=me + dm)))
        messages.append(shift(
            base + 2, there, back_there,
            remote(source, target.at[1], side_send.at[base + 2], side_recv.at[base + 2], grp=grp + dg)))
    messages.append(shift(8, has_right, has_left, remote(
        pack.at[pl.ds(half, half)], from_left, side_send.at[8], side_recv.at[8], mem=me + 1)))
    messages.append(shift(9, has_left, has_right, remote(
        pack.at[pl.ds(0, half)], from_right, side_send.at[9], side_recv.at[9], mem=me - 1)))

    for arrived in messages:
        arrived()

    for i in range(layers):
        x = i - halo
        region = 0 if x < 0 else (1 if x < edge else 2)
        x = x % edge
        p, k = divmod(x, 2)
        q, t = divmod(p, 2)
        own = pairs[p] if region == 1 else (from_left[p - half] if region == 0 else from_right[p])
        below = roll(from_below[region, q], -halo * (1 - t) - edge * k, 1)
        above = roll(from_above[region, q], edge + halo - edge * k - halo * t, 1)
        value = jnp.where(z < halo, below,
                          jnp.where(z >= halo + edge, above, roll(own, halo - edge * k, 1)))
        level[0, i] = value
        sign[i] = value * lax.rsqrt(value * value + 1.0)

    always = me < columns

    def row_ahead(x):
        return jnp.where(lane >= LANES - wide, roll(x, -1, 0), x)

    ahead_y = [row_ahead(roll(mask, -wide, 1)) for mask in masks_y]
    ahead_z = [roll(mask, -1, 1) for mask in masks_z]

    def steepest(side, behind, ahead):
        most = jnp.maximum(jnp.maximum(side * behind, -(side * ahead)), 0.0)
        return most * most

    def sweep(step, low, high):
        now, later = step % 2, (step + 1) % 2

        @pl.when(always)
        def _():
            for k, shift_by in enumerate((wide, -wide, 1, -1)):
                for i in range(low, high):
                    turned[k, i] = roll(level[now, i], shift_by, 1)

        @pl.when(always)
        def _():
            gap = None
            for i in range(low, high):
                region = 0 if i < halo else (1 if i < halo + edge else 2)
                value, field = level[now, i], sign[i]
                side = jnp.where(field > 0, 1.0, -1.0)

                def across(j):
                    change = level[now, j] - level[now, j - 1]
                    if j == halo:
                        change = change * link_x[0]
                    elif j == halo + edge:
                        change = change * link_x[1]
                    return change

                gap = across(i) if gap is None else gap
                ahead = across(i + 1)
                squares = steepest(side, gap, ahead)
                gap = ahead
                before = turned[0, i]
                before = jnp.where(lane < wide, roll(before, 1, 0), before)
                squares = squares + steepest(side, (value - before) * masks_y[region],
                                             (row_ahead(turned[1, i]) - value) * ahead_y[region])
                squares = squares + steepest(side, (value - turned[2, i]) * masks_z[region],
                                             (turned[3, i] - value) * ahead_z[region]) + EPSILON
                level[later, i] = value - TIME_STEP * field * (squares * lax.rsqrt(squares) - 1.0)

    for step in range(STEPS):
        sweep(step, step + 1, layers - 1 - step)

    last = STEPS % 2
    final = []
    for pair in range(edge // 2):
        one, two = level[last, halo + 2 * pair], level[last, halo + 2 * pair + 1]
        final.append(jnp.where(z < edge, roll(one, -halo, 1), roll(two, edge - halo, 1)))
    back[...] = dot(depart, pieces(jnp.concatenate(final, axis=1), 0),
                    ((1,), (0,))).reshape(back.shape)
    sent += begin_exchange(back, home, back_send, back_recv, True)
    end_exchange(back, home, back_send, back_recv)

    owned = dot(living, pieces(home[...].reshape(-1, home.shape[2]), 0), ((0,), (0,))).T
    for pair in range(edge // 2):
        for y in range(edge):
            for k in range(2):
                at = ((pair * edge + y) * 2 + k) * edge
                out_ref[2 * pair + k, y] = owned[at:at + edge]
    for copy in sent:
        copy.wait_send()
    for there, copy in late:
        pl.when(there)(copy.wait_send)


def on_device(phi_owned, band_counts, neighbours):
    edge, own_slots = phi_owned.shape[0], phi_owned.shape[3]
    columns, groups = lax.axis_size("mem"), lax.axis_size("grp")
    tiles = neighbours.shape[2]
    rows = tiles // columns
    padded = -(-own_slots // (8 * columns)) * 8
    halo, cells = STEPS, edge * edge * edge
    anywhere = pl.BlockSpec(memory_space=pltpu.HBM)
    buffer = pltpu.VMEM((columns, padded, cells), F32)
    table = pltpu.VMEM((6, 1, tiles), jnp.int32)
    pair = lambda *lead: pltpu.VMEM((*lead, rows, LANES), F32)
    slots, layers = edge // 4, edge + 2 * halo
    return pl.pallas_call(
        functools.partial(kernel, columns, groups),
        out_shape=jax.ShapeDtypeStruct(phi_owned.shape, F32),
        in_specs=[anywhere] * 3,
        out_specs=pl.BlockSpec(memory_space=pltpu.VMEM),
        scratch_shapes=[
            pltpu.VMEM(phi_owned.shape, F32), pltpu.SMEM(band_counts.shape, jnp.int32),
            table, table, table,
        ] + [buffer] * 4 + [
            pair(edge // 2), pair(slots), pair(slots), pair(3, slots), pair(3, slots),
            pair(edge // 4), pair(edge // 4), pair(2, layers), pair(layers), pair(4, layers),
            pltpu.SemaphoreType.DMA((3,)),
        ] + [pltpu.SemaphoreType.DMA((columns,))] * 4 + [pltpu.SemaphoreType.DMA((10,))] * 2,
        compiler_params=pltpu.CompilerParams(
            collective_id=0, has_side_effects=True, vmem_limit_bytes=16 * 1024 * 1024),
    )(*[pltpu.with_memory_space_constraint(x, pltpu.HBM)
        for x in (phi_owned, band_counts, jnp.transpose(neighbours, (1, 0, 2)))])


def solution(mesh):
    return jax.shard_map(
        on_device,
        mesh=mesh,
        in_specs=(P(None, None, None, ("grp", "mem")), P("grp", None), P("grp", None, None)),
        out_specs=P(None, None, None, ("grp", "mem")),
        check_vma=False,
    )
```

```python
import functools

import jax
import jax.numpy as jnp
from jax import lax
from jax.experimental import pallas as pl
from jax.experimental.pallas import tpu as pltpu
from jax.sharding import PartitionSpec as P

STEPS = 4
TIME_STEP = 0.5
EPSILON = 1e-06
LANES = 128
F32 = jnp.float32
BF16 = jnp.bfloat16


def roll(x, shift, axis):
    shift = shift % x.shape[axis]
    return x if shift == 0 else pltpu.roll(x, shift, axis)


def pieces(x, axis):
    high = x.astype(BF16)
    rest = x - high.astype(F32)
    middle = rest.astype(BF16)
    low = (rest - middle.astype(F32)).astype(BF16)
    return jnp.concatenate([high, middle, low], axis=axis)


def dot(a, b, dims):
    return lax.dot_general(a, b, (dims, ((), ())), preferred_element_type=F32)


def kernel(
    columns, groups, phi_hbm, counts_hbm, links_hbm, out_ref,
    phi_ref, counts_ref, links_own, links_below, links_above,
    leave, land, back, home, pack, up, down, from_below, from_above, from_left, from_right,
    level, sign, turned, slopes, in_sem, out_send, out_recv, back_send, back_recv, side_send, side_recv,
):
    edge = phi_ref.shape[0]
    own_slots = phi_ref.shape[3]
    padded, tiles = leave.shape[1], links_own.shape[2]
    rows = tiles // columns
    halo = STEPS
    wide = 2 * edge
    layers = edge + 2 * halo
    me, grp = lax.axis_index("mem"), lax.axis_index("grp")
    has_left, has_right = me > 0, me < columns - 1
    has_below, has_above = grp > 0, grp < groups - 1
    across_grp = [(-1, has_below), (1, has_above)]
    across_mem = [(-1, has_left), (1, has_right)]
    distances = range(1, columns)

    fetch = [
        pltpu.make_async_copy(phi_hbm, phi_ref, in_sem.at[0]),
        pltpu.make_async_copy(counts_hbm, counts_ref, in_sem.at[1]),
        pltpu.make_async_copy(links_hbm, links_own, in_sem.at[2]),
    ]
    for copy in fetch:
        copy.start()

    barrier = pltpu.get_barrier_semaphore()

    def greet(**peer):
        pl.semaphore_signal(barrier, inc=1, device_id=peer, device_id_type=pl.DeviceIdType.MESH)

    for d in sorted(distances, key=lambda d: -min(d, columns - d)):
        greet(mem=lax.rem(me + d, columns))
    greetings = jnp.int32(columns - 1)
    for dg, there in across_grp:
        for dm, beside in across_mem + [(0, True)]:
            both = jnp.logical_and(there, beside)
            greetings = greetings + both.astype(jnp.int32)

            @pl.when(both)
            def _():
                greet(grp=grp + dg, mem=me + dm)

    def remote(source, target, send, recv, **peer):
        return pltpu.make_async_remote_copy(
            src_ref=source, dst_ref=target, send_sem=send, recv_sem=recv,
            device_id=peer, device_id_type=pl.DeviceIdType.MESH)

    early = 2

    def turn(i, favour):
        if not favour:
            return lax.rem(me + 1 + i, columns)
        if i == 0:
            return jnp.where(me == 0, 1, 0)
        rest = early + lax.rem(me + columns - 3 * early + i + 1, columns - early)
        return jnp.where(me < early, i + 1, 1 if i == 1 else rest)

    def begin_exchange(source, target, send, recv, favour=False):
        started = []
        for i in range(columns - 1):
            peer = turn(i, favour)
            d = lax.rem(peer - me + columns, columns)
            copy = remote(source.at[peer], target.at[me], send.at[d], recv.at[d], mem=peer)
            copy.start()
            started.append(copy)
        target[me] = source[me]
        return started

    def end_exchange(source, target, send, recv):
        for d in reversed(distances):
            origin = lax.rem(me + columns - d, columns)
            remote(source.at[origin], target.at[origin], send.at[d], recv.at[d],
                   mem=origin).wait_recv()

    late = []

    def shift(index, condition, sources, copy):
        pl.when(condition)(copy.start)
        late.append((condition, copy))
        return lambda: pl.when(sources)(copy.wait_recv)

    fetch[1].wait()
    count_of = [counts_ref[0, m] for m in range(columns)]
    first, count = jnp.int32(0), jnp.int32(0)
    for m in range(columns):
        first = first + jnp.where(m < me, count_of[m], 0)
        count = count + jnp.where(m == me, count_of[m], 0)
    entries = columns * padded
    slot = lax.broadcasted_iota(jnp.int32, (1, own_slots), 1)
    key = (first + slot) % columns * padded + slot // columns
    chosen = lax.broadcasted_iota(jnp.int32, (entries, own_slots), 0) == key
    placing = jnp.where(chosen, 1.0, 0.0).astype(F32)

    fetch[0].wait()
    cells = jnp.concatenate(
        [phi_ref[2 * pair + k, y] for pair in range(edge // 2) for y in range(edge) for k in range(2)],
        axis=0)
    leave[...] = dot(jnp.concatenate([placing.astype(BF16)] * 3, axis=1), pieces(cells, 1),
                     ((1,), (1,))).reshape(leave.shape)
    fetch[2].wait()

    pl.semaphore_wait(barrier, greetings)
    sent = begin_exchange(leave, land, out_send, out_recv)
    tables = [
        shift(0, has_above, has_below, remote(
            links_own, links_below, side_send.at[0], side_recv.at[0], grp=grp + 1)),
        shift(1, has_below, has_above, remote(
            links_own, links_above, side_send.at[1], side_recv.at[1], grp=grp - 1)),
    ]

    def blank(absent, *views):
        @pl.when(jnp.logical_not(absent))
        def _():
            for ref, value in views:
                ref[...] = jnp.full_like(ref, value)

    blank(has_left, (from_left, 0.0))
    blank(has_right, (from_right, 0.0))
    for there, table, ref in ((has_below, links_below, from_below), (has_above, links_above, from_above)):
        blank(there, (table, -1), (ref.at[1], 0.0))
        blank(jnp.logical_and(there, has_left), (ref.at[0], 0.0))
        blank(jnp.logical_and(there, has_right), (ref.at[2], 0.0))

    def arrival(dims, axis):
        entry = lax.broadcasted_iota(jnp.int32, dims, axis)
        block, place = entry // padded, entry % padded
        start, length = jnp.zeros(dims, jnp.int32), jnp.zeros(dims, jnp.int32)
        for m in range(columns):
            start = start + jnp.where(block > m, count_of[m], 0)
            length = length + jnp.where(block == m, count_of[m], 0)
        shape = (rows, entries) if axis == 1 else (entries, rows)
        offset = lax.broadcasted_iota(jnp.int32, shape, 1 - axis) * columns + me - start
        begin = place * columns
        return jnp.where((offset >= begin) & (offset < begin + columns) & (offset < length),
                         1.0, 0.0).astype(F32).astype(BF16)

    arrive = jnp.concatenate([arrival((1, entries), 1)] * 3, axis=1)
    depart = jnp.concatenate([arrival((entries, 1), 0)] * 3, axis=1)
    living = jnp.concatenate([jnp.where(slot < count, placing, 0.0).astype(BF16)] * 3, axis=0)

    lane = lax.broadcasted_iota(jnp.int32, (rows, LANES), 1)
    z = lane % wide
    tile_of = (lax.broadcasted_iota(jnp.int32, (rows, tiles), 1)
               - lax.broadcasted_iota(jnp.int32, (rows, tiles), 0) * columns - me)
    held = {dm: tile_of == dm for dm in (-1, 0, 1)}

    for arrived in tables:
        arrived()

    def link(table, face, dm):
        there = jnp.where(table[face] >= 0, 1.0, 0.0).astype(F32)
        value = jnp.sum(jnp.where(held[dm], there, 0.0), axis=1, keepdims=True)
        return jnp.broadcast_to(value, (rows, LANES))

    def layered(face, dm):
        return jnp.where(z < halo, link(links_below, face, dm),
                         jnp.where(z >= halo + edge, link(links_above, face, dm),
                                   link(links_own, face, dm)))

    link_x = [layered(0, 0), layered(1, 0)]
    masks_y = [jnp.where(lane < wide, layered(2, dm), 1.0) for dm in (-1, 0, 1)]
    masks_z = [jnp.where(z == halo, link(links_own, 4, dm),
                         jnp.where(z == halo + edge, link(links_own, 5, dm),
                                   jnp.where(z == 0, 0.0, 1.0))) for dm in (-1, 0, 1)]

    end_exchange(leave, land, out_send, out_recv)
    packed = dot(arrive, pieces(land[...].reshape(-1, land.shape[2]), 0), ((1,), (0,)))
    pairs = [packed[:, p * LANES:(p + 1) * LANES] for p in range(edge // 2)]
    for p, both in enumerate(pairs):
        pack[p] = both
    low = lane % edge < halo
    slots = up.shape[0]
    for q in range(slots):
        here, after = pairs[2 * q], pairs[2 * q + 1]
        up[q] = jnp.where(low, roll(after, -halo, 1), here)
        down[q] = jnp.where(low, here, roll(after, halo, 1))

    half = edge // 4
    messages = []
    for dg, there, back_there, source, target, base in (
        (1, has_above, has_below, up, from_below, 2), (-1, has_below, has_above, down, from_above, 5),
    ):
        for k, (dm, beside, back_beside, part) in enumerate((
            (1, has_right, has_left, slots - 1), (-1, has_left, has_right, 0),
        )):
            messages.append(shift(
                base + k, jnp.logical_and(there, beside), jnp.logical_and(back_there, back_beside),
                remote(source.at[part], target.at[1 - dm, part], side_send.at[base + k],
                       side_recv.at[base + k], grp=grp + dg, mem=me + dm)))
        messages.append(shift(
            base + 2, there, back_there,
            remote(source, target.at[1], side_send.at[base + 2], side_recv.at[base + 2], grp=grp + dg)))
    messages.append(shift(8, has_right, has_left, remote(
        pack.at[pl.ds(half, half)], from_left, side_send.at[8], side_recv.at[8], mem=me + 1)))
    messages.append(shift(9, has_left, has_right, remote(
        pack.at[pl.ds(0, half)], from_right, side_send.at[9], side_recv.at[9], mem=me - 1)))

    for arrived in messages:
        arrived()

    for i in range(layers):
        x = i - halo
        region = 0 if x < 0 else (1 if x < edge else 2)
        x = x % edge
        p, k = divmod(x, 2)
        q, t = divmod(p, 2)
        own = pairs[p] if region == 1 else (from_left[p - half] if region == 0 else from_right[p])
        below = roll(from_below[region, q], -halo * (1 - t) - edge * k, 1)
        above = roll(from_above[region, q], edge + halo - edge * k - halo * t, 1)
        value = jnp.where(z < halo, below,
                          jnp.where(z >= halo + edge, above, roll(own, halo - edge * k, 1)))
        level[0, i] = value
        sign[i] = value * lax.rsqrt(value * value + 1.0)

    always = me < columns

    def row_ahead(x):
        return jnp.where(lane >= LANES - wide, roll(x, -1, 0), x)

    ahead_y = [row_ahead(roll(mask, -wide, 1)) for mask in masks_y]
    ahead_z = [roll(mask, -1, 1) for mask in masks_z]

    def steepest(side, behind, ahead):
        most = jnp.maximum(jnp.maximum(side * behind, -(side * ahead)), 0.0)
        return most * most

    def sweep(step, low, high):
        now, later = step % 2, (step + 1) % 2

        @pl.when(always)
        def _():
            for k, shift_by in enumerate((wide, -wide, 1, -1)):
                for i in range(low, high):
                    turned[k, i] = roll(level[now, i], shift_by, 1)

            def across(j):
                change = level[now, j] - level[now, j - 1]
                if j == halo:
                    change = change * link_x[0]
                elif j == halo + edge:
                    change = change * link_x[1]
                return change

            gap = across(low)
            for i in range(low, high):
                ahead = across(i + 1)
                slopes[i] = steepest(jnp.where(sign[i] > 0, 1.0, -1.0), gap, ahead)
                gap = ahead

        @pl.when(always)
        def _():
            for i in range(low, high):
                region = 0 if i < halo else (1 if i < halo + edge else 2)
                value, field = level[now, i], sign[i]
                side = jnp.where(field > 0, 1.0, -1.0)
                before = turned[0, i]
                before = jnp.where(lane < wide, roll(before, 1, 0), before)
                squares = slopes[i] + steepest(side, (value - before) * masks_y[region],
                                               (row_ahead(turned[1, i]) - value) * ahead_y[region])
                squares = squares + steepest(side, (value - turned[2, i]) * masks_z[region],
                                             (turned[3, i] - value) * ahead_z[region]) + EPSILON
                level[later, i] = value - TIME_STEP * field * (squares * lax.rsqrt(squares) - 1.0)

    for step in range(STEPS):
        sweep(step, step + 1, layers - 1 - step)

    last = STEPS % 2
    low_half = [roll(level[last, halo + 2 * p], -halo, 1) for p in range(edge // 2)]
    high_half = [roll(level[last, halo + 2 * p + 1], edge - halo, 1) for p in range(edge // 2)]
    final = [jnp.where(z < edge, one, two) for one, two in zip(low_half, high_half)]
    back[...] = dot(depart, pieces(jnp.concatenate(final, axis=1), 0),
                    ((1,), (0,))).reshape(back.shape)
    sent += begin_exchange(back, home, back_send, back_recv, True)
    end_exchange(back, home, back_send, back_recv)

    owned = dot(living, pieces(home[...].reshape(-1, home.shape[2]), 0), ((0,), (0,))).T
    for pair in range(edge // 2):
        for y in range(edge):
            for k in range(2):
                at = ((pair * edge + y) * 2 + k) * edge
                out_ref[2 * pair + k, y] = owned[at:at + edge]
    for copy in sent:
        copy.wait_send()
    for there, copy in late:
        pl.when(there)(copy.wait_send)


def on_device(phi_owned, band_counts, neighbours):
    edge, own_slots = phi_owned.shape[0], phi_owned.shape[3]
    columns, groups = lax.axis_size("mem"), lax.axis_size("grp")
    tiles = neighbours.shape[2]
    rows = tiles // columns
    padded = -(-own_slots // (8 * columns)) * 8
    halo, cells = STEPS, edge * edge * edge
    anywhere = pl.BlockSpec(memory_space=pltpu.HBM)
    buffer = pltpu.VMEM((columns, padded, cells), F32)
    table = pltpu.VMEM((6, 1, tiles), jnp.int32)
    pair = lambda *lead: pltpu.VMEM((*lead, rows, LANES), F32)
    slots, layers = edge // 4, edge + 2 * halo
    return pl.pallas_call(
        functools.partial(kernel, columns, groups),
        out_shape=jax.ShapeDtypeStruct(phi_owned.shape, F32),
        in_specs=[anywhere] * 3,
        out_specs=pl.BlockSpec(memory_space=pltpu.VMEM),
        scratch_shapes=[
            pltpu.VMEM(phi_owned.shape, F32), pltpu.SMEM(band_counts.shape, jnp.int32),
            table, table, table,
        ] + [buffer] * 4 + [
            pair(edge // 2), pair(slots), pair(slots), pair(3, slots), pair(3, slots),
            pair(edge // 4), pair(edge // 4), pair(2, layers), pair(layers), pair(4, layers), pair(layers),
            pltpu.SemaphoreType.DMA((3,)),
        ] + [pltpu.SemaphoreType.DMA((columns,))] * 4 + [pltpu.SemaphoreType.DMA((10,))] * 2,
        compiler_params=pltpu.CompilerParams(
            collective_id=0, has_side_effects=True, vmem_limit_bytes=16 * 1024 * 1024),
    )(*[pltpu.with_memory_space_constraint(x, pltpu.HBM)
        for x in (phi_owned, band_counts, jnp.transpose(neighbours, (1, 0, 2)))])


def solution(mesh):
    return jax.shard_map(
        on_device,
        mesh=mesh,
        in_specs=(P(None, None, None, ("grp", "mem")), P("grp", None), P("grp", None, None)),
        out_specs=P(None, None, None, ("grp", "mem")),
        check_vma=False,
    )
```
